32 devices in a mesh: dp: 4 (over z), expert: 8 (over y, x, core).
Axes of the slice: x: 2, y: 2, z: 4, core: 2. Of those that a mesh axis runs over, the one named last changes fastest.
Arguments:
- tokens: bfloat16 [512, 7168], P('expert'), may hold values from -6 to 6
- routes: int32 [512, 8], P('expert'), may hold values from 0 to 7, all different within a row; in each aligned block of 64 rows (0 to 63, 64 to 127, ...) at most 64 rows name the same one
- route_weight: int32 [512, 8], P('expert'), may hold values from 1 to 4096
- w_gate: bfloat16 [8, 7168, 2048], P('expert', None, 'dp'), may hold values from -0.0625 to 0.0625
- w_up: bfloat16 [8, 7168, 2048], P('expert', None, 'dp'), may hold values from -0.0625 to 0.0625
- w_down: bfloat16 [8, 2048, 7168], P('expert', 'dp'), may hold values from -0.125 to 0.125
- prev_inputs: bfloat16 [4, 8, 64, 7168], P('dp', 'expert'), may hold values from -6 to 6
Outputs:
- mixed: bfloat16 [512, 7168], P('expert', 'dp')
- hessian: float32 [7168, 8, 128], P('dp', 'expert')
The draws below stay inside these ranges and needn't reach their ends.
Inputs may be any that keep to these rules, and one draw needn't show every extreme that they name: `routes`: in each aligned block of 64 rows (the rows of one index of expert) no expert is named more than 64 times, a bound that some block reaches; the 8 experts of a token differ.
All inputs are finite; a program needn't handle non-finite values.
Results may differ from the reference program's by a relative error of at most 0.014.
Values may be sent and summed in bfloat16 or wider, within the bound.
A program may use at most 128 MiB of HBM per device.

```python
import math
import jax
import jax.numpy as jnp
import numpy as np
from jax import lax

D = 7168
FF = 2048
TOP = 8
TOK_DEV = 64
PREV_ROWS = 64
HESS_COLS = 128
EXPERTS = 8
TOKENS = 512
CAP = 64
N_DP = 4
N_EXPERT = 8


def with_ends(result, rng, smallest, largest):
    shape = result.shape
    spot = [jax.random.randint(jax.random.fold_in(rng, axis), (), 0, shape[axis]) for axis in range(len(shape))]
    result = result.at[tuple(spot)].set(smallest)
    longest = shape.index(max(shape))
    spot[longest] = (spot[longest] + 1) % shape[longest]
    return result.at[tuple(spot)].set(largest)


def block_scale(rng, extent, pieces, low, top_value):
    def one(position, blocks):
        steps = jax.random.uniform(jax.random.fold_in(jax.random.fold_in(rng, 6), position), (blocks,), jnp.float32, low / len(pieces), top_value / len(pieces))
        return jnp.repeat(jnp.exp(steps), extent[position] // blocks).reshape((-1,) + (1,) * (len(extent) - position - 1))

    level = one(*pieces[0])
    for cut in pieces[1:]:
        level = level * one(*cut)
    return level


def shared_out(own_key, own, number, rows, number_of, top, bound, skew):
    order = jax.random.permutation(own_key, number_of)
    crowded, usual = load_shares(number_of, rows * top, bound, skew, True), load_shares(number_of, rows * top, bound, skew, False)
    places = jnp.arange(number_of)

    def named(lengths, offset_by):
        used = int((lengths > 0).sum())
        fixed = max(1, used // 4)
        moved = fixed + (places - fixed + offset_by * (used - fixed)) % max(1, number_of - fixed)
        return jnp.zeros((number_of,), jnp.int32).at[order[jnp.where(places < fixed, places, moved)]].set(jnp.asarray(lengths, jnp.int32))

    lengths = jnp.where(number % 4 == 0, named(crowded, number // 4), named(usual, number - number // 4 - 1))
    mixed = jax.random.permutation(jax.random.fold_in(own, 3), number_of)
    giver, sink = mixed[0:number_of // 2 * 2:2], mixed[1:number_of // 2 * 2:2]
    margin = jnp.minimum(lengths[giver] - 1, bound - lengths[sink]) // 2
    margin = jnp.where((giver == order[0]) | (sink == order[0]) | (lengths[sink] == 0), 0, jnp.maximum(margin, 0))
    moved = jax.random.randint(jax.random.fold_in(own, 4), (number_of // 2,), 0, 1 << 20) % (margin + 1)
    lengths = lengths.at[giver].add(-moved).at[sink].add(moved)
    labels = jnp.searchsorted(jnp.cumsum(lengths), jnp.arange(rows * top), side="right").astype(jnp.int32)
    listing = labels.reshape(top, rows).T
    listing = listing[jax.random.permutation(jax.random.fold_in(own, 1), rows)]
    offset_by = jax.random.randint(jax.random.fold_in(own, 2), (rows, 1), 0, top)
    return jnp.take_along_axis(listing, (jnp.arange(top)[None, :] + offset_by) % top, axis=1)


def load_shares(amount, total, reach, lean, full):
    portions = [(1 << 20) // math.isqrt(grade ** lean) + 1 for grade in range(1, amount + 1)]
    largest = reach if full else min(reach, max(-(-total // amount), total * portions[0] // sum(portions)))
    least = 1 if total - largest >= amount - 1 else 0
    holding, surplus = [largest] + [least] * (amount - 1), total - largest - least * (amount - 1)
    while surplus > 0:
        candidates = [i for i in range(1, amount) if holding[i] < largest] or [i for i in range(1, amount) if holding[i] < reach]
        pool, budget = sum([portions[i] for i in candidates]), surplus
        for i in candidates:
            addition = min(reach - holding[i], max(1, budget * portions[i] // pool), surplus)
            holding[i] = holding[i] + addition
            surplus = surplus - addition
    return np.array(holding)


def centred(key, extent, width, most, shards=(), held_as=jnp.bfloat16):
    gain = block_scale(key, extent, shards, -0.22, 0.18) if shards else 1.0
    values = jax.random.normal(key, extent, jnp.float32) * width * gain
    return jnp.minimum(jnp.maximum(values, -most), most).astype(held_as)


def setup_inputs(seed: int = 0) -> dict:
    keys = jax.random.split(jax.random.key(seed), 8)
    tokens = centred(keys[0], (TOKENS, D), 1.0, 6.0, ((0, 8),))
    routes_keys = jax.random.split(jax.random.fold_in(keys[1], 1), TOKENS // TOK_DEV)
    routes_turns = jax.random.permutation(jax.random.fold_in(keys[1], 3), TOKENS // TOK_DEV)
    routes = jax.vmap(lambda own, number: shared_out(jax.random.fold_in(keys[1], 2), own, number, TOK_DEV, EXPERTS, TOP, CAP, 2))(routes_keys, routes_turns).reshape((TOKENS, TOP))
    route_weight = with_ends(jax.random.randint(keys[2], (TOKENS, TOP), 1, 4097), jax.random.fold_in(keys[2], 1), 1, 4096).astype(jnp.int32)
    w_gate = centred(keys[3], (EXPERTS, D, FF), D ** -0.5, 0.0625, ((0, 8), (2, 4)))
    w_up = centred(keys[4], (EXPERTS, D, FF), D ** -0.5, 0.0625, ((0, 8), (2, 4)))
    w_down = centred(keys[5], (EXPERTS, FF, D), FF ** -0.5, 0.125, ((0, 8), (1, 4)))
    prev_inputs = centred(keys[6], (N_DP, EXPERTS, PREV_ROWS, D), 1.0, 6.0, ((0, 4), (1, 8)))
    return {"tokens": tokens, "routes": routes, "route_weight": route_weight, "w_gate": w_gate, "w_up": w_up, "w_down": w_down, "prev_inputs": prev_inputs}


def route_slots(flat_ids):
    onehot = (flat_ids[:, None] == jnp.arange(EXPERTS, dtype=jnp.int32)[None, :]).astype(jnp.int32)
    earlier = jnp.cumsum(onehot, axis=0) - onehot
    return jnp.sum(earlier * onehot, axis=1).astype(jnp.int32)


def reference(tokens, routes, route_weight, w_gate, w_up, w_down, prev_inputs):
    blocks = routes.reshape(N_EXPERT, TOK_DEV * TOP).astype(jnp.int32)
    slots = jax.vmap(route_slots)(blocks)
    anchor = jnp.arange(N_EXPERT, dtype=jnp.int32)[:, None]
    places = ((blocks * N_EXPERT + anchor) * CAP + slots).astype(jnp.int32)
    token_ids = jnp.arange(TOKENS, dtype=jnp.int32).reshape(N_EXPERT, TOK_DEV, 1)
    token_ids = jnp.broadcast_to(token_ids, (N_EXPERT, TOK_DEV, TOP)).reshape(N_EXPERT, TOK_DEV * TOP)
    table = jnp.full((EXPERTS * N_EXPERT * CAP,), TOKENS, jnp.int32)
    table = table.at[places.reshape(-1)].set(token_ids.reshape(-1)).reshape(EXPERTS, N_EXPERT * CAP)
    padded = jnp.concatenate([tokens, jnp.zeros((1, D), tokens.dtype)], axis=0)
    slice_width = FF // N_DP

    def one_expert(item):
        index, gate_w, up_w, down_w = item
        rows = padded[index]
        gate = jnp.dot(rows, gate_w, preferred_element_type=jnp.float32)
        up = jnp.dot(rows, up_w, preferred_element_type=jnp.float32)
        hidden = (jax.nn.silu(gate) * up).astype(jnp.bfloat16)
        total = jnp.zeros((N_EXPERT * CAP, D), jnp.float32)
        for group in range(N_DP):
            piece = jnp.dot(hidden[:, group * slice_width:(group + 1) * slice_width],
                            down_w[group * slice_width:(group + 1) * slice_width],
                            preferred_element_type=jnp.float32).astype(jnp.bfloat16)
            total = total + lax.optimization_barrier(piece).astype(jnp.float32)
        return total

    outputs = lax.map(one_expert, (table, w_gate, w_up, w_down))
    flat_out = outputs.reshape(EXPERTS * N_EXPERT * CAP, D)
    picked = flat_out[places.reshape(-1)].reshape(TOKENS, TOP, D)
    counts = route_weight.astype(jnp.float32)
    shares = 2.5 * counts / jnp.sum(counts, axis=1, keepdims=True)
    mixed = jnp.sum(picked * shares[:, :, None], axis=1).astype(jnp.bfloat16)

    def one_gram(history):
        rows = history.reshape(N_DP * PREV_ROWS, D)
        gram = jnp.dot(rows.T, rows[:, :HESS_COLS], preferred_element_type=jnp.float32)
        return gram * (2.0 / (N_DP * PREV_ROWS))

    grams = lax.map(one_gram, jnp.moveaxis(prev_inputs, 1, 0))
    hessian = jnp.transpose(grams, (1, 0, 2))
    return mixed, hessian
```

```python
import functools

import jax
import jax.numpy as jnp
from jax import lax
from jax.experimental import pallas as pl
from jax.experimental.pallas import tpu as pltpu
from jax.sharding import PartitionSpec as P

HESS_COLS = 128


def route_slots(flat_ids, experts_all):
    onehot = (flat_ids[:, None] == jnp.arange(experts_all, dtype=jnp.int32)[None, :]).astype(
        jnp.int32
    )
    earlier = jnp.cumsum(onehot, axis=0) - onehot
    return jnp.sum(earlier * onehot, axis=1)


def combine_rows(back, places, shares, tok_dev, top):
    columns = back.shape[-1]
    rows = back.reshape(-1, columns)[places]
    weighted = rows.astype(jnp.float32) * shares.reshape(-1, 1)
    return jnp.sum(weighted.reshape(tok_dev, top, columns), axis=1)


def route_shares(route_weight):
    weight_counts = route_weight.astype(jnp.float32)
    return 2.5 * weight_counts / jnp.sum(weight_counts, axis=1, keepdims=True)


def gram_window(prev_inputs, n_dp, width):
    history = prev_inputs.reshape(prev_inputs.shape[1], prev_inputs.shape[2], width)
    head_cols = history[:, :, :HESS_COLS]
    gram_scale = 2.0 / (n_dp * history.shape[1])
    return lax.psum_scatter(
        (
            jnp.einsum("jrd,jrh->djh", history, head_cols, preferred_element_type=jnp.float32)
            * gram_scale
        ).astype(jnp.bfloat16),
        "dp",
        scatter_dimension=0,
        tiled=True,
    ).astype(jnp.float32)


def slotted(tokens, routes, route_weight, w_gate, w_up, w_down):
    tok_dev, top = routes.shape
    exp_dev = w_gate.shape[0]
    width = tokens.shape[1]
    n_expert = lax.axis_size("expert")
    experts_all = exp_dev * n_expert
    capacity = min(tok_dev, tok_dev * top * 5 // (4 * experts_all))
    flat_ids = routes.reshape(-1)
    slots = route_slots(flat_ids, experts_all)
    places = flat_ids * capacity + slots
    shares = route_shares(route_weight)
    picks = jnp.arange(experts_all * capacity, dtype=jnp.int32)[:, None] == places[None, :]
    placing = jnp.any(picks.reshape(experts_all * capacity, tok_dev, top), axis=2).astype(
        jnp.bfloat16
    )
    outgoing = jnp.dot(placing, tokens, preferred_element_type=jnp.float32).astype(jnp.bfloat16)
    outgoing = outgoing.reshape(experts_all, capacity, width)
    arrived = lax.all_to_all(outgoing, "expert", split_axis=0, concat_axis=0, tiled=True)
    arrived = arrived.reshape(n_expert, exp_dev, capacity, width)
    gate = jnp.einsum("sjcd,jdf->sjcf", arrived, w_gate, preferred_element_type=jnp.float32)
    up = jnp.einsum("sjcd,jdf->sjcf", arrived, w_up, preferred_element_type=jnp.float32)
    hidden = (jax.nn.silu(gate) * up).astype(jnp.bfloat16)
    partial_out = jnp.einsum("sjcf,jfd->sjcd", hidden, w_down, preferred_element_type=jnp.float32)
    partial_out = partial_out.astype(jnp.bfloat16)
    back = lax.all_to_all(
        partial_out.reshape(experts_all, capacity, width),
        "expert",
        split_axis=0,
        concat_axis=0,
        tiled=True,
    )
    own_sum = combine_rows(back, places, shares, tok_dev, top)
    return lax.psum_scatter(own_sum.astype(jnp.bfloat16), "dp", scatter_dimension=1, tiled=True)

LANES = 128
MESH = pl.DeviceIdType.MESH


def flip(index, bit):
    return index + bit - 2 * bit * ((index // bit) % 2)


def dense_kernel(
    n_dp,
    n_expert,
    tokens,
    share_in,
    w_gate,
    w_up,
    w_down,
    prev,
    mixed_ref,
    hess_ref,
    xall,
    share_all,
    wg,
    wu,
    wd,
    g_acc,
    u_acc,
    hid,
    mine,
    sb0,
    rb0,
    sb1,
    rb1,
    sb2,
    rb2,
    sb3,
    rb3,
    hx,
    hh,
    lsem,
    send_sem,
    recv_sem,
):
    me = lax.axis_index("expert")
    my_dp = lax.axis_index("dp")
    core, xx, yy = me % 2, (me // 2) % 2, (me // 4) % 2
    peer, ex, ey = flip(me, 1), flip(me, 2), flip(me, 4)
    ed = flip(ex, 4)
    chunks, depth = xall.shape[0], xall.shape[-1]
    rows = xall.shape[3]
    half = rows // 2
    cols = rb3.shape[-1]
    hidden_w = wg.shape[-1]
    counter = [0]
    local_counter = [0]

    def local(src, dst):
        copy = pltpu.make_async_copy(src, dst, lsem.at[local_counter[0]])
        local_counter[0] += 1
        copy.start()
        return copy

    def remote(src, dst, where):
        copy = pltpu.make_async_remote_copy(
            src_ref=src,
            dst_ref=dst,
            send_sem=send_sem.at[counter[0]],
            recv_sem=recv_sem.at[counter[0]],
            device_id=where,
            device_id_type=MESH,
        )
        counter[0] += 1
        copy.start()
        sent.append(copy)
        return copy

    sent = []
    token_loads = [
        local(tokens.at[:, c * depth : (c + 1) * depth], xall.at[c, core, me // 2])
        for c in range(chunks)
    ]
    hist_own = local(prev.at[:, pl.ds(pl.multiple_of(my_dp * cols, LANES), cols)], hx.at[0])
    head_own = local(prev.at[:, 0:HESS_COLS], hh.at[0])
    share_own = local(share_in, share_all.at[core, me // 2])
    gate_loads, up_loads = [], []
    for c in range(chunks):
        gate_loads.append(local(w_gate.at[c * depth : (c + 1) * depth, :], wg.at[c]))
        up_loads.append(local(w_up.at[c * depth : (c + 1) * depth, :], wu.at[c]))
    turns = [n_dp // 2] + [d for d in range(1, n_dp) if d != n_dp // 2] + [0]
    down_loads = []
    for i, d in enumerate(turns):
        start = pl.multiple_of(((my_dp + d) % n_dp) * cols, LANES)
        down_loads.append(local(w_down.at[:, pl.ds(start, cols)], wd.at[i]))

    barrier = pltpu.get_barrier_semaphore()
    for d in range(1, n_expert):
        pl.semaphore_signal(
            barrier, inc=1, device_id={"expert": (me + d) % n_expert}, device_id_type=MESH
        )
    for d in range(1, n_dp):
        pl.semaphore_signal(
            barrier, inc=1, device_id={"dp": (my_dp + d) % n_dp}, device_id_type=MESH
        )
    pl.semaphore_wait(barrier, n_expert + n_dp - 2)

    to_peer, to_x, to_y = {"expert": peer}, {"expert": ex}, {"expert": ey}
    flow = {}

    def block(c, who):
        return xall.at[c, who % 2, who // 2]

    def own(c):
        token_loads[c].wait()
        for name, where in (("x", to_x), ("y", to_y), ("p", to_peer)):
            flow[c, name] = remote(block(c, me), block(c, me), where)

    def relay(c):
        flow[c, "x"].wait_recv()
        flow[c, "d0"] = remote(block(c, ex).at[0:half], block(c, ex).at[0:half], to_y)
        flow[c, "px"] = remote(block(c, ex), block(c, ex), to_peer)
        flow[c, "y"].wait_recv()
        flow[c, "d1"] = remote(block(c, ey).at[half:rows], block(c, ey).at[half:rows], to_x)
        flow[c, "py"] = remote(block(c, ey), block(c, ey), to_peer)

    def corner(c):
        flow[c, "d0"].wait_recv()
        flow[c, "p0"] = remote(block(c, ed).at[0:half], block(c, ed).at[0:half], to_peer)
        flow[c, "d1"].wait_recv()
        flow[c, "p1"] = remote(block(c, ed).at[half:rows], block(c, ed).at[half:rows], to_peer)

    tile = 2 * LANES

    def widen(c):
        for name in ("p", "px", "py", "p0", "p1"):
            flow[c, name].wait_recv()
        gate_loads[c].wait()
        up_loads[c].wait()

        @pl.loop(0, hidden_w // tile)
        def _(n):
            at = pl.ds(pl.multiple_of(n * tile, tile), tile)
            x = xall[c].reshape(n_expert * rows, depth)
            g = jnp.dot(x, wg[c, :, at], preferred_element_type=jnp.float32)
            u = jnp.dot(x, wu[c, :, at], preferred_element_type=jnp.float32)
            if c == 0:
                g_acc[:, at] = g
                u_acc[:, at] = u
            else:
                g_acc[:, at] += g
                u_acc[:, at] += u

    own(0)
    share_own.wait()
    share_flows = [
        remote(
            share_all.at[core, me // 2],
            share_all.at[core, me // 2],
            {"expert": (me + d) % n_expert},
        )
        for d in range(1, n_expert)
    ]
    hist_flows = []
    for d in range(1, n_dp):
        start = pl.multiple_of(((my_dp + d) % n_dp) * cols, LANES)
        where = {"dp": (my_dp + d) % n_dp}
        hist_flows.append(remote(prev.at[:, pl.ds(start, cols)], hx.at[d], where))
        hist_flows.append(remote(prev.at[:, 0:HESS_COLS], hh.at[d], where))

    for c in range(chunks + 2):
        if 1 <= c < chunks:
            own(c)
        if 1 <= c <= chunks:
            relay(c - 1)
        if 2 <= c:
            corner(c - 2)
            if c == chunks + 1:
                hist_own.wait()
                head_own.wait()
                for copy in hist_flows:
                    copy.wait_recv()
                scale = 2.0 / (n_dp * hx.shape[1])

                @pl.loop(0, cols // tile)
                def _(n):
                    at = pl.multiple_of(n * tile, tile)
                    left = hx[:, :, pl.ds(at, tile)].reshape(n_dp * hx.shape[1], tile)
                    right = hh[...].reshape(n_dp * hx.shape[1], HESS_COLS)
                    gram = lax.dot_general(
                        left, right, (((0,), (0,)), ((), ())), preferred_element_type=jnp.float32
                    )
                    hess_ref[pl.ds(at, tile), :] = gram * scale

                for copy in share_flows:
                    copy.wait_recv()
            widen(c - 2)

    for kind in range(2):
        span = slice(kind * n_expert // 2 * rows, (kind + 1) * n_expert // 2 * rows)
        sh = share_all[kind].reshape(n_expert // 2 * rows, LANES)
        lane = lax.broadcasted_iota(jnp.int32, sh.shape, 1)
        own_share = jnp.sum(jnp.where(lane == me, sh, 0.0), axis=1, keepdims=True)
        g = g_acc[span, :]
        hid[kind] = (g / (1.0 + jnp.exp(-g)) * u_acc[span, :] * own_share).astype(jnp.bfloat16)

    stage = {}
    chips = n_expert // 2

    def down(i):
        down_loads[i].wait()

        @pl.loop(0, cols // tile)
        def _(n):
            at = pl.ds(pl.multiple_of(n * tile, tile), tile)
            out = jnp.dot(hid[1 - core], wd[i, :, at], preferred_element_type=jnp.float32)
            sb0[i, :, :, at] = out.astype(jnp.bfloat16).reshape(chips, rows, tile)

        stage[i, 0] = remote(sb0.at[i], rb0.at[i], to_peer)

        @pl.loop(0, cols // tile)
        def _(n):
            at = pl.ds(pl.multiple_of(n * tile, tile), tile)
            out = jnp.dot(hid[core], wd[i, :, at], preferred_element_type=jnp.float32)
            mine[i, :, :, at] = out.reshape(chips, rows, tile)

    low, high = slice(0, half), slice(half, rows)

    def both(i, chip, part):
        return mine[i, chip, part, :] + rb0[i, chip, part, :].astype(jnp.float32)

    def first(i):
        stage[i, 0].wait_recv()
        for k in range(2):
            sb1[i, 0, k] = both(i, k * 2 + 1 - xx, low).astype(jnp.bfloat16)
        stage[i, 1] = remote(sb1.at[i, 0], rb1.at[i, 0], to_x)
        for k in range(2):
            sb1[i, 1, k] = both(i, (1 - yy) * 2 + k, high).astype(jnp.bfloat16)
        stage[i, 2] = remote(sb1.at[i, 1], rb1.at[i, 1], to_y)

    def second(i):
        stage[i, 1].wait_recv()
        out = both(i, (1 - yy) * 2 + xx, low) + rb1[i, 0, 1 - yy].astype(jnp.float32)
        sb2[i, 0] = out.astype(jnp.bfloat16)
        stage[i, 3] = remote(sb2.at[i, 0], rb2.at[i, 0], to_y)
        stage[i, 2].wait_recv()
        out = both(i, yy * 2 + 1 - xx, high) + rb1[i, 1, 1 - xx].astype(jnp.float32)
        sb2[i, 1] = out.astype(jnp.bfloat16)
        stage[i, 4] = remote(sb2.at[i, 1], rb2.at[i, 1], to_x)

    def third(i):
        d = turns[i]
        chip = me // 2
        stage[i, 3].wait_recv()
        stage[i, 4].wait_recv()
        top = both(i, chip, low) + rb1[i, 0, yy].astype(jnp.float32)
        top = top + rb2[i, 0].astype(jnp.float32)
        end = both(i, chip, high) + rb1[i, 1, xx].astype(jnp.float32)
        end = end + rb2[i, 1].astype(jnp.float32)
        if d:
            sb3[d - 1, low, :] = top.astype(jnp.bfloat16)
            sb3[d - 1, high, :] = end.astype(jnp.bfloat16)
            stage[i, 5] = remote(
                sb3.at[d - 1], rb3.at[d - 1], {"dp": (my_dp + d) % n_dp}
            )
        else:
            for j, other in enumerate(turns):
                if other:
                    stage[j, 5].wait_recv()
                    top = top + rb3[other - 1, low, :].astype(jnp.float32)
                    end = end + rb3[other - 1, high, :].astype(jnp.float32)
            mixed_ref[low, :] = top.astype(jnp.bfloat16)
            mixed_ref[high, :] = end.astype(jnp.bfloat16)

    for step in range(n_dp + 4):
        if step < n_dp:
            down(step)
        if 1 <= step <= n_dp:
            first(step - 1)
        if 3 <= step < n_dp + 3:
            second(step - 3)
        if 4 <= step:
            third(step - 4)
    for copy in sent:
        copy.wait_send()


def everyone(tokens, routes, route_weight, w_gate, w_up, w_down, prev_inputs):
    rows, width = tokens.shape
    n_expert = lax.axis_size("expert")
    n_dp = lax.axis_size("dp")
    hidden_w = w_gate.shape[2]
    shares = route_shares(route_weight)
    named = routes[:, :, None] == jnp.arange(LANES, dtype=jnp.int32)[None, None, :]
    by_expert = jnp.sum(jnp.where(named, shares[:, :, None], 0.0), axis=1)
    prev = prev_inputs.reshape(prev_inputs.shape[2], width)
    cols = width // n_dp
    chunks = 4
    depth = width // chunks
    chips = n_expert // 2
    total = n_expert * rows
    bf16, f32 = jnp.bfloat16, jnp.float32
    copies = 9 * chunks + (n_expert - 1) + 2 * (n_dp - 1) + 5 * n_dp + n_dp - 1
    vmem = pl.BlockSpec(memory_space=pltpu.VMEM)
    hbm = pl.BlockSpec(memory_space=pl.ANY)
    mixed, hess = pl.pallas_call(
        functools.partial(dense_kernel, n_dp, n_expert),
        out_shape=(
            jax.ShapeDtypeStruct((rows, cols), bf16),
            jax.ShapeDtypeStruct((cols, HESS_COLS), f32),
        ),
        in_specs=[hbm] * 6,
        out_specs=(vmem, vmem),
        scratch_shapes=[
            pltpu.VMEM((chunks, 2, chips, rows, depth), bf16),
            pltpu.VMEM((2, chips, rows, LANES), f32),
            pltpu.VMEM((chunks, depth, hidden_w), bf16),
            pltpu.VMEM((chunks, depth, hidden_w), bf16),
            pltpu.VMEM((n_dp, hidden_w, cols), bf16),
            pltpu.VMEM((total, hidden_w), f32),
            pltpu.VMEM((total, hidden_w), f32),
            pltpu.VMEM((2, total // 2, hidden_w), bf16),
            pltpu.VMEM((n_dp, chips, rows, cols), f32),
            pltpu.VMEM((n_dp, chips, rows, cols), bf16),
            pltpu.VMEM((n_dp, chips, rows, cols), bf16),
            pltpu.VMEM((n_dp, 2, 2, rows // 2, cols), bf16),
            pltpu.VMEM((n_dp, 2, 2, rows // 2, cols), bf16),
            pltpu.VMEM((n_dp, 2, rows // 2, cols), bf16),
            pltpu.VMEM((n_dp, 2, rows // 2, cols), bf16),
            pltpu.VMEM((n_dp - 1, rows, cols), bf16),
            pltpu.VMEM((n_dp - 1, rows, cols), bf16),
            pltpu.VMEM((n_dp, prev.shape[0], cols), bf16),
            pltpu.VMEM((n_dp, prev.shape[0], HESS_COLS), bf16),
            pltpu.SemaphoreType.DMA((3 * chunks + n_dp + 3,)),
            pltpu.SemaphoreType.DMA((copies,)),
            pltpu.SemaphoreType.DMA((copies,)),
        ],
        compiler_params=pltpu.CompilerParams(
            collective_id=0, has_side_effects=True, vmem_limit_bytes=67043328
        ),
        name="dense_layer",
    )(tokens, by_expert, w_gate[0], w_up[0], w_down[0], prev)
    return mixed, hess.reshape(cols, 1, HESS_COLS)


def shards(tokens, routes, route_weight, w_gate, w_up, w_down, prev_inputs):
    n_expert = lax.axis_size("expert")
    if w_gate.shape[0] == 1 and routes.shape[1] == n_expert == 2 * 2 * 2:
        return everyone(tokens, routes, route_weight, w_gate, w_up, w_down, prev_inputs)
    hessian = gram_window(prev_inputs, lax.axis_size("dp"), tokens.shape[1])
    return slotted(tokens, routes, route_weight, w_gate, w_up, w_down), hessian


def solution(mesh):
    placed = (
        P("expert", None),
        P("expert", None),
        P("expert", None),
        P("expert", None, "dp"),
        P("expert", None, "dp"),
        P("expert", "dp", None),
        P("dp", "expert", None, None),
    )
    return jax.shard_map(
        shards,
        mesh=mesh,
        in_specs=placed,
        out_specs=(P("expert", "dp"), P("dp", "expert", None)),
        check_vma=False,
    )
```

```python
import functools

import jax
import jax.numpy as jnp
from jax import lax
from jax.experimental import pallas as pl
from jax.experimental.pallas import tpu as pltpu
from jax.sharding import PartitionSpec as P

HESS_COLS = 128


def route_slots(flat_ids, experts_all):
    onehot = (flat_ids[:, None] == jnp.arange(experts_all, dtype=jnp.int32)[None, :]).astype(
        jnp.int32
    )
    earlier = jnp.cumsum(onehot, axis=0) - onehot
    return jnp.sum(earlier * onehot, axis=1)


def combine_rows(back, places, shares, tok_dev, top):
    columns = back.shape[-1]
    rows = back.reshape(-1, columns)[places]
    weighted = rows.astype(jnp.float32) * shares.reshape(-1, 1)
    return jnp.sum(weighted.reshape(tok_dev, top, columns), axis=1)


def route_shares(route_weight):
    weight_counts = route_weight.astype(jnp.float32)
    return 2.5 * weight_counts / jnp.sum(weight_counts, axis=1, keepdims=True)


def gram_window(prev_inputs, n_dp, width):
    history = prev_inputs.reshape(prev_inputs.shape[1], prev_inputs.shape[2], width)
    head_cols = history[:, :, :HESS_COLS]
    gram_scale = 2.0 / (n_dp * history.shape[1])
    return lax.psum_scatter(
        (
            jnp.einsum("jrd,jrh->djh", history, head_cols, preferred_element_type=jnp.float32)
            * gram_scale
        ).astype(jnp.bfloat16),
        "dp",
        scatter_dimension=0,
        tiled=True,
    ).astype(jnp.float32)


def slotted(tokens, routes, route_weight, w_gate, w_up, w_down):
    tok_dev, top = routes.shape
    exp_dev = w_gate.shape[0]
    width = tokens.shape[1]
    n_expert = lax.axis_size("expert")
    experts_all = exp_dev * n_expert
    capacity = min(tok_dev, tok_dev * top * 5 // (4 * experts_all))
    flat_ids = routes.reshape(-1)
    slots = route_slots(flat_ids, experts_all)
    places = flat_ids * capacity + slots
    shares = route_shares(route_weight)
    picks = jnp.arange(experts_all * capacity, dtype=jnp.int32)[:, None] == places[None, :]
    placing = jnp.any(picks.reshape(experts_all * capacity, tok_dev, top), axis=2).astype(
        jnp.bfloat16
    )
    outgoing = jnp.dot(placing, tokens, preferred_element_type=jnp.float32).astype(jnp.bfloat16)
    outgoing = outgoing.reshape(experts_all, capacity, width)
    arrived = lax.all_to_all(outgoing, "expert", split_axis=0, concat_axis=0, tiled=True)
    arrived = arrived.reshape(n_expert, exp_dev, capacity, width)
    gate = jnp.einsum("sjcd,jdf->sjcf", arrived, w_gate, preferred_element_type=jnp.float32)
    up = jnp.einsum("sjcd,jdf->sjcf", arrived, w_up, preferred_element_type=jnp.float32)
    hidden = (jax.nn.silu(gate) * up).astype(jnp.bfloat16)
    partial_out = jnp.einsum("sjcf,jfd->sjcd", hidden, w_down, preferred_element_type=jnp.float32)
    partial_out = partial_out.astype(jnp.bfloat16)
    back = lax.all_to_all(
        partial_out.reshape(experts_all, capacity, width),
        "expert",
        split_axis=0,
        concat_axis=0,
        tiled=True,
    )
    own_sum = combine_rows(back, places, shares, tok_dev, top)
    return lax.psum_scatter(own_sum.astype(jnp.bfloat16), "dp", scatter_dimension=1, tiled=True)

LANES = 128
MESH = pl.DeviceIdType.MESH


def flip(index, bit):
    return index + bit - 2 * bit * ((index // bit) % 2)


def dense_kernel(
    n_dp,
    n_expert,
    tokens,
    share_in,
    w_gate,
    w_up,
    w_down,
    prev,
    mixed_ref,
    hess_ref,
    xall,
    share_all,
    wg,
    wu,
    wd,
    g_acc,
    u_acc,
    hid,
    mine,
    sb0,
    rb0,
    sb1,
    rb1,
    sb2,
    rb2,
    sb3,
    rb3,
    hx,
    hh,
    lsem,
    send_sem,
    recv_sem,
):
    me = lax.axis_index("expert")
    my_dp = lax.axis_index("dp")
    core, xx, yy = me % 2, (me // 2) % 2, (me // 4) % 2
    peer, ex, ey = flip(me, 1), flip(me, 2), flip(me, 4)
    ed = flip(ex, 4)
    chunks, depth = xall.shape[0], xall.shape[-1]
    rows = xall.shape[3]
    half = rows // 2
    cols = rb3.shape[-1]
    hidden_w = wg.shape[-1]
    counter = [0]
    local_counter = [0]

    def local(src, dst):
        copy = pltpu.make_async_copy(src, dst, lsem.at[local_counter[0]])
        local_counter[0] += 1
        copy.start()
        return copy

    def remote(src, dst, where):
        copy = pltpu.make_async_remote_copy(
            src_ref=src,
            dst_ref=dst,
            send_sem=send_sem.at[counter[0]],
            recv_sem=recv_sem.at[counter[0]],
            device_id=where,
            device_id_type=MESH,
        )
        counter[0] += 1
        copy.start()
        sent.append(copy)
        return copy

    sent = []
    side = my_dp % 2
    last = chunks - 1

    def piece(c):
        return pl.ds(pl.multiple_of((side * last + c * (1 - 2 * side)) * depth, LANES), depth)

    token_loads = [
        local(tokens.at[:, piece(c)], xall.at[c, core, me // 2]) for c in range(chunks)
    ]
    hist_own = local(prev.at[:, pl.ds(pl.multiple_of(my_dp * cols, LANES), cols)], hx.at[0])
    head_own = local(prev.at[:, 0:HESS_COLS], hh.at[0])
    share_own = local(share_in, share_all.at[core, me // 2])
    gate_loads, up_loads = [], []
    for c in range(chunks):
        gate_loads.append(local(w_gate.at[piece(c), :], wg.at[c]))
        up_loads.append(local(w_up.at[piece(c), :], wu.at[c]))
    turns = [n_dp // 2] + [d for d in range(1, n_dp) if d != n_dp // 2] + [0]
    down_loads = []
    for i, d in enumerate(turns):
        start = pl.multiple_of(((my_dp + d) % n_dp) * cols, LANES)
        down_loads.append(local(w_down.at[:, pl.ds(start, cols)], wd.at[i]))

    barrier = pltpu.get_barrier_semaphore()
    for d in range(1, n_expert):
        pl.semaphore_signal(
            barrier, inc=1, device_id={"expert": (me + d) % n_expert}, device_id_type=MESH
        )
    for d in range(1, n_dp):
        pl.semaphore_signal(
            barrier, inc=1, device_id={"dp": (my_dp + d) % n_dp}, device_id_type=MESH
        )
    pl.semaphore_wait(barrier, n_expert + n_dp - 2)

    to_z = {"dp": flip(my_dp, 1)}
    to_peer, to_x, to_y = {"expert": peer}, {"expert": ex}, {"expert": ey}
    flow = {}

    def block(c, who):
        return xall.at[c, who % 2, who // 2]

    def own(c):
        token_loads[c].wait()
        ways = (("x", to_x), ("y", to_y), ("p", to_peer))
        for name, where in ways if c < last else ways[2:]:
            flow[c, name] = remote(block(c, me), block(c, me), where)

    def across(who):
        return remote(block(0, who), block(last, who), to_z)

    def relay(c):
        if c == last:
            for name, who in (("x", ex), ("y", ey), ("d", ed)):
                flow["z" + name].wait_recv()
                flow[c, "p" + name] = remote(block(c, who), block(c, who), to_peer)
            return
        flow[c, "x"].wait_recv()
        flow[c, "d0"] = remote(block(c, ex).at[0:half], block(c, ex).at[0:half], to_y)
        if c == 0:
            flow["zx"] = across(ex)
        flow[c, "px"] = remote(block(c, ex), block(c, ex), to_peer)
        flow[c, "y"].wait_recv()
        flow[c, "d1"] = remote(block(c, ey).at[half:rows], block(c, ey).at[half:rows], to_x)
        if c == 0:
            flow["zy"] = across(ey)
        flow[c, "py"] = remote(block(c, ey), block(c, ey), to_peer)

    def corner(c):
        if c == last:
            return
        flow[c, "d0"].wait_recv()
        flow[c, "p0"] = remote(block(c, ed).at[0:half], block(c, ed).at[0:half], to_peer)
        flow[c, "d1"].wait_recv()
        flow[c, "p1"] = remote(block(c, ed).at[half:rows], block(c, ed).at[half:rows], to_peer)
        if c == 0:
            flow["zd"] = across(ed)

    tile = 2 * LANES

    def widen(c):
        for name in ("p", "px", "py", "p0", "p1") if c < last else ("p", "px", "py", "pd"):
            flow[c, name].wait_recv()
        gate_loads[c].wait()
        up_loads[c].wait()

        @pl.loop(0, hidden_w // tile)
        def _(n):
            at = pl.ds(pl.multiple_of(n * tile, tile), tile)
            x = xall[c].reshape(n_expert * rows, depth)
            g = jnp.dot(x, wg[c, :, at], preferred_element_type=jnp.float32)
            u = jnp.dot(x, wu[c, :, at], preferred_element_type=jnp.float32)
            if c == 0:
                g_acc[:, at] = g
                u_acc[:, at] = u
            else:
                g_acc[:, at] += g
                u_acc[:, at] += u

    own(0)
    share_own.wait()
    share_flows = [
        remote(
            share_all.at[core, me // 2],
            share_all.at[core, me // 2],
            {"expert": (me + d) % n_expert},
        )
        for d in range(1, n_expert)
    ]
    hist_flows = []

    def send_history():
        for d in range(1, n_dp):
            start = pl.multiple_of(((my_dp + d) % n_dp) * cols, LANES)
            where = {"dp": (my_dp + d) % n_dp}
            hist_flows.append(remote(prev.at[:, pl.ds(start, cols)], hx.at[d], where))
            hist_flows.append(remote(prev.at[:, 0:HESS_COLS], hh.at[d], where))

    for c in range(chunks + 2):
        if 1 <= c < chunks:
            own(c)
        if 1 <= c <= chunks:
            relay(c - 1)
        if 2 <= c:
            corner(c - 2)
            if c == 2:
                send_history()
            widen(c - 2)

    for copy in share_flows:
        copy.wait_recv()
    for kind in range(2):
        span = slice(kind * n_expert // 2 * rows, (kind + 1) * n_expert // 2 * rows)
        sh = share_all[kind].reshape(n_expert // 2 * rows, LANES)
        lane = lax.broadcasted_iota(jnp.int32, sh.shape, 1)
        own_share = jnp.sum(jnp.where(lane == me, sh, 0.0), axis=1, keepdims=True)
        g = g_acc[span, :]
        hid[kind] = (g / (1.0 + jnp.exp(-g)) * u_acc[span, :] * own_share).astype(jnp.bfloat16)

    stage = {}
    chips = n_expert // 2

    def down(i):
        down_loads[i].wait()

        @pl.loop(0, cols // tile)
        def _(n):
            at = pl.ds(pl.multiple_of(n * tile, tile), tile)
            out = jnp.dot(hid[1 - core], wd[i, :, at], preferred_element_type=jnp.float32)
            sb0[i, :, :, at] = out.astype(jnp.bfloat16).reshape(chips, rows, tile)

        stage[i, 0] = remote(sb0.at[i], rb0.at[i], to_peer)

    def keep(i):
        @pl.loop(0, cols // tile)
        def _(n):
            at = pl.ds(pl.multiple_of(n * tile, tile), tile)
            out = jnp.dot(hid[core], wd[i, :, at], preferred_element_type=jnp.float32)
            mine[i, :, :, at] = out.reshape(chips, rows, tile)

    low, high = slice(0, half), slice(half, rows)

    def both(i, chip, part):
        return mine[i, chip, part, :] + rb0[i, chip, part, :].astype(jnp.float32)

    def first(i):
        stage[i, 0].wait_recv()
        for k in range(2):
            sb1[i, 0, k] = both(i, k * 2 + 1 - xx, low).astype(jnp.bfloat16)
        stage[i, 1] = remote(sb1.at[i, 0], rb1.at[i, 0], to_x)
        for k in range(2):
            sb1[i, 1, k] = both(i, (1 - yy) * 2 + k, high).astype(jnp.bfloat16)
        stage[i, 2] = remote(sb1.at[i, 1], rb1.at[i, 1], to_y)

    def second(i):
        stage[i, 1].wait_recv()
        out = both(i, (1 - yy) * 2 + xx, low) + rb1[i, 0, 1 - yy].astype(jnp.float32)
        sb2[i, 0] = out.astype(jnp.bfloat16)
        stage[i, 3] = remote(sb2.at[i, 0], rb2.at[i, 0], to_y)
        stage[i, 2].wait_recv()
        out = both(i, yy * 2 + 1 - xx, high) + rb1[i, 1, 1 - xx].astype(jnp.float32)
        sb2[i, 1] = out.astype(jnp.bfloat16)
        stage[i, 4] = remote(sb2.at[i, 1], rb2.at[i, 1], to_x)

    def third(i):
        d = turns[i]
        chip = me // 2
        stage[i, 3].wait_recv()
        stage[i, 4].wait_recv()
        top = both(i, chip, low) + rb1[i, 0, yy].astype(jnp.float32)
        top = top + rb2[i, 0].astype(jnp.float32)
        end = both(i, chip, high) + rb1[i, 1, xx].astype(jnp.float32)
        end = end + rb2[i, 1].astype(jnp.float32)
        if d:
            sb3[d - 1, low, :] = top.astype(jnp.bfloat16)
            sb3[d - 1, high, :] = end.astype(jnp.bfloat16)
            stage[i, 5] = remote(
                sb3.at[d - 1], rb3.at[d - 1], {"dp": (my_dp + d) % n_dp}
            )
        else:
            for j, other in enumerate(turns):
                if other:
                    stage[j, 5].wait_recv()
                    top = top + rb3[other - 1, low, :].astype(jnp.float32)
                    end = end + rb3[other - 1, high, :].astype(jnp.float32)
            mixed_ref[low, :] = top.astype(jnp.bfloat16)
            mixed_ref[high, :] = end.astype(jnp.bfloat16)

    def gram():
        hist_own.wait()
        head_own.wait()
        for copy in hist_flows:
            copy.wait_recv()
        scale = 2.0 / (n_dp * hx.shape[1])

        @pl.loop(0, cols // tile)
        def _(n):
            at = pl.multiple_of(n * tile, tile)
            left = hx[:, :, pl.ds(at, tile)].reshape(n_dp * hx.shape[1], tile)
            right = hh[...].reshape(n_dp * hx.shape[1], HESS_COLS)
            product = lax.dot_general(
                left, right, (((0,), (0,)), ((), ())), preferred_element_type=jnp.float32
            )
            hess_ref[pl.ds(at, tile), :] = product * scale

    for step in range(n_dp + 4):
        if step < n_dp:
            down(step)
        if 1 <= step <= n_dp:
            keep(step - 1)
            first(step - 1)
        if step == n_dp + 1:
            gram()
        if 3 <= step < n_dp + 3:
            second(step - 3)
        if 4 <= step:
            third(step - 4)
    for copy in sent:
        copy.wait_send()


def everyone(tokens, routes, route_weight, w_gate, w_up, w_down, prev_inputs):
    rows, width = tokens.shape
    n_expert = lax.axis_size("expert")
    n_dp = lax.axis_size("dp")
    hidden_w = w_gate.shape[2]
    shares = route_shares(route_weight)
    named = routes[:, :, None] == jnp.arange(LANES, dtype=jnp.int32)[None, None, :]
    by_expert = jnp.sum(jnp.where(named, shares[:, :, None], 0.0), axis=1)
    prev = prev_inputs.reshape(prev_inputs.shape[2], width)
    cols = width // n_dp
    chunks = 4
    depth = width // chunks
    chips = n_expert // 2
    total = n_expert * rows
    bf16, f32 = jnp.bfloat16, jnp.float32
    copies = 9 * chunks + (n_expert - 1) + 2 * (n_dp - 1) + 5 * n_dp + n_dp - 1
    vmem = pl.BlockSpec(memory_space=pltpu.VMEM)
    hbm = pl.BlockSpec(memory_space=pl.ANY)
    mixed, hess = pl.pallas_call(
        functools.partial(dense_kernel, n_dp, n_expert),
        out_shape=(
            jax.ShapeDtypeStruct((rows, cols), bf16),
            jax.ShapeDtypeStruct((cols, HESS_COLS), f32),
        ),
        in_specs=[hbm] * 6,
        out_specs=(vmem, vmem),
        scratch_shapes=[
            pltpu.VMEM((chunks, 2, chips, rows, depth), bf16),
            pltpu.VMEM((2, chips, rows, LANES), f32),
            pltpu.VMEM((chunks, depth, hidden_w), bf16),
            pltpu.VMEM((chunks, depth, hidden_w), bf16),
            pltpu.VMEM((n_dp, hidden_w, cols), bf16),
            pltpu.VMEM((total, hidden_w), f32),
            pltpu.VMEM((total, hidden_w), f32),
            pltpu.VMEM((2, total // 2, hidden_w), bf16),
            pltpu.VMEM((n_dp, chips, rows, cols), f32),
            pltpu.VMEM((n_dp, chips, rows, cols), bf16),
            pltpu.VMEM((n_dp, chips, rows, cols), bf16),
            pltpu.VMEM((n_dp, 2, 2, rows // 2, cols), bf16),
            pltpu.VMEM((n_dp, 2, 2, rows // 2, cols), bf16),
            pltpu.VMEM((n_dp, 2, rows // 2, cols), bf16),
            pltpu.VMEM((n_dp, 2, rows // 2, cols), bf16),
            pltpu.VMEM((n_dp - 1, rows, cols), bf16),
            pltpu.VMEM((n_dp - 1, rows, cols), bf16),
            pltpu.VMEM((n_dp, prev.shape[0], cols), bf16),
            pltpu.VMEM((n_dp, prev.shape[0], HESS_COLS), bf16),
            pltpu.SemaphoreType.DMA((3 * chunks + n_dp + 3,)),
            pltpu.SemaphoreType.DMA((copies,)),
            pltpu.SemaphoreType.DMA((copies,)),
        ],
        compiler_params=pltpu.CompilerParams(
            collective_id=0, has_side_effects=True, vmem_limit_bytes=67043328
        ),
        name="dense_layer",
    )(tokens, by_expert, w_gate[0], w_up[0], w_down[0], prev)
    return mixed, hess.reshape(cols, 1, HESS_COLS)


def shards(tokens, routes, route_weight, w_gate, w_up, w_down, prev_inputs):
    n_expert = lax.axis_size("expert")
    if w_gate.shape[0] == 1 and routes.shape[1] == n_expert == 2 * 2 * 2:
        return everyone(tokens, routes, route_weight, w_gate, w_up, w_down, prev_inputs)
    hessian = gram_window(prev_inputs, lax.axis_size("dp"), tokens.shape[1])
    return slotted(tokens, routes, route_weight, w_gate, w_up, w_down), hessian


def solution(mesh):
    placed = (
        P("expert", None),
        P("expert", None),
        P("expert", None),
        P("expert", None, "dp"),
        P("expert", None, "dp"),
        P("expert", "dp", None),
        P("dp", "expert", None, None),
    )
    return jax.shard_map(
        shards,
        mesh=mesh,
        in_specs=placed,
        out_specs=(P("expert", "dp"), P("dp", "expert", None)),
        check_vma=False,
    )
```
